32 devices in a mesh: row: 8 (over z, y), col: 4 (over x, core).
Axes of the slice: x: 2, y: 2, z: 4, core: 2. Of those that a mesh axis runs over, the one named last changes fastest.
Arguments:
- fields: float32 [1, 4, 256, 256, 256], P(None, None, 'row', 'col'), may hold values from -6 to 6
- cotangent: float32 [1, 4, 256, 256, 256], P(None, None, 'row', 'col'), may hold values from -6 to 6
- spec_weights: float32 [2, 4, 4, 16, 16, 16], replicated, may hold values from -96 to 96
- point_weights: float32 [4, 4], replicated, may hold values from -3 to 3
- bias: float32 [4], replicated, may hold values from -3 to 3
Outputs:
- grad_fields: float32 [1, 4, 256, 256, 256], P(None, None, 'row', 'col')
- grad_spectral: float32 [2, 4, 4, 16, 16, 16], replicated
The draws below stay inside these ranges and needn't reach their ends.
All inputs are finite; a program needn't handle non-finite values.
Results may differ from the reference program's by a relative error of at most 0.00011.
Values sent between devices are 32-bit elements; how exact they have to be, the bound alone decides.
A program may use at most 128 MiB of HBM per device.

```python
import jax
import jax.numpy as jnp
from jax import lax

B = 1
C = 4
NX = 256
NY = 256
NZ = 256
MX = 16
MY = 16
MZ = 16


def block_levels(rng, shape, shards, smallest, top_value):
    factor_of, own = 1.0, jax.random.fold_in(rng, 6)
    for axis_at, parts in shards:
        draws = jnp.exp(jax.random.uniform(jax.random.fold_in(own, axis_at), (parts,), jnp.float32, smallest / len(shards), top_value / len(shards)))
        factor_of = factor_of * jnp.repeat(draws, shape[axis_at] // parts).reshape([-1 if axis == axis_at else 1 for axis in range(len(shape))])
    return factor_of


def gaussian(rng, extent, scale, most, cuts=(), kind=jnp.bfloat16):
    loudness = block_levels(rng, extent, cuts, -0.22, 0.18) if cuts else 1.0
    entries = jax.random.normal(rng, extent, jnp.float32) * scale * loudness
    return jnp.minimum(jnp.maximum(entries, -most), most).astype(kind)


def setup_inputs(seed: int = 0) -> dict:
    splits = jax.random.split(jax.random.key(seed), 6)
    return {
        "fields": gaussian(splits[0], (B, C, NY, NZ, NX), 1.0, 6.0, ((2, 8), (3, 4)), jnp.float32),
        "cotangent": gaussian(splits[1], (B, C, NY, NZ, NX), 1.0, 6.0, ((2, 8), (3, 4)), jnp.float32),
        "spec_weights": gaussian(splits[2], (2, C, C, MX, MY, MZ), ((NX * NY * NZ / (4.0 * C * MX * MY * MZ)) ** 0.5), 96.0, (), jnp.float32),
        "point_weights": gaussian(splits[3], (C, C), C ** -0.5, 3.0, (), jnp.float32),
        "bias": gaussian(splits[4], (C,), 0.5, 3.0, (), jnp.float32),
    }


def crop(spectrum):
    spectrum = spectrum[..., :MX]
    spectrum = jnp.concatenate([spectrum[..., :MY // 2, :, :], spectrum[..., NY - MY // 2:, :, :]], axis=-3)
    spectrum = jnp.concatenate([spectrum[..., :MZ // 2, :], spectrum[..., NZ - MZ // 2:, :]], axis=-2)
    return spectrum

def expand(modes):
    lead = modes.shape[:2]
    modes = jnp.pad(modes, [(0, 0), (0, 0), (0, 0), (0, 0), (0, NX // 2 + 1 - MX)])
    width_x = modes.shape[4]
    zeros_z = jnp.zeros(lead + (MY, NZ - MZ, width_x), modes.dtype)
    modes = jnp.concatenate([modes[..., :MZ // 2, :], zeros_z, modes[..., MZ // 2:, :]], axis=-2)
    zeros_y = jnp.zeros(lead + (NY - MY, NZ, width_x), modes.dtype)
    modes = jnp.concatenate([modes[..., :MY // 2, :, :], zeros_y, modes[..., MY // 2:, :, :]], axis=-3)
    return modes

def spectral(fields, spec_weights):
    spectrum = crop(jnp.fft.rfftn(fields, axes=(2, 3, 4)))
    weights = spec_weights[0] + 1j * spec_weights[1]
    mixed_modes = jnp.einsum('biqrp,iopqr->boqrp', spectrum, weights, precision=lax.Precision.HIGHEST)
    return jnp.fft.irfftn(expand(mixed_modes), s=(NY, NZ, NX), axes=(2, 3, 4))

def reference(fields, cotangent, spec_weights, point_weights, bias):

    def forward(field_in, weight_in):
        local_term = jnp.einsum('bcyzx,co->boyzx', field_in, point_weights, precision=lax.Precision.HIGHEST)
        pre_activation = spectral(field_in, weight_in) + local_term + bias[None, :, None, None, None]
        return jax.nn.gelu(pre_activation, approximate=False)
    output, pullback = jax.vjp(forward, fields, spec_weights)
    grad_fields, grad_spectral = pullback(cotangent.astype(output.dtype))
    return (grad_fields, grad_spectral)
```

```python
import functools
import math

import jax
import jax.numpy as jnp
import numpy as np
from jax import lax
from jax.experimental import pallas as pl
from jax.experimental.pallas import tpu as pltpu
from jax.sharding import PartitionSpec as P

f32 = jnp.float32
bf16 = jnp.bfloat16
MESH = pl.DeviceIdType.MESH
TILE = 256


def split(value):
    high = value.astype(bf16)
    return high, (value - high.astype(f32)).astype(bf16)


def split_np(value):
    value = np.asarray(value, np.float32)
    high = value.astype(jnp.bfloat16)
    low = (value - high.astype(np.float32)).astype(jnp.bfloat16)
    return high, low


def signed(number):
    wave = np.arange(number)
    return np.where(wave < number // 2, wave, wave - number)


def x_tables(chans, length, modes, cells):
    angle = 2.0 * np.pi / length * ((np.arange(length)[:, None] * np.arange(modes)) % length)
    first = np.concatenate([np.cos(angle), -np.sin(angle)], 1)
    weight = np.where(np.arange(modes) == 0, 1.0, 2.0) / cells
    last = np.concatenate([np.cos(angle) * weight, -np.sin(angle) * weight], 1).T
    eye = np.eye(chans)
    wide = (eye[:, None, :, None] * first[None, :, None, :]).reshape(chans * length, -1)
    high, low = split_np(wide)
    analysis = np.concatenate([high, low], 1)
    analysis = np.concatenate([analysis, analysis], 0)
    tall = (eye[:, None, :, None] * last[None, :, None, :]).reshape(-1, chans * length)
    high, low = split_np(tall)
    return analysis, np.concatenate([high, high, low], 0)


def yz_tables(ny, nz, my, mz):
    ang_y = 2.0 * np.pi / ny * ((np.arange(ny)[:, None] * signed(my)) % ny)
    ang_z = 2.0 * np.pi / nz * ((np.arange(nz)[:, None] * signed(mz)) % nz)
    tab_y = np.concatenate([np.repeat(np.cos(ang_y), mz, 1), np.repeat(np.sin(ang_y), mz, 1)], 1)
    tab_z = np.concatenate([np.tile(np.cos(ang_z), (1, my)), np.tile(np.sin(ang_z), (1, my))], 1)
    return tab_y.astype(np.float32), tab_z.astype(np.float32)


def dot(a, b):
    return jnp.dot(a, b, preferred_element_type=f32)


def dot_nt(a, b):
    return lax.dot_general(a, b, (((1,), (1,)), ((), ())), preferred_element_type=f32)


def analyse(split_x, w_ref, t_ref, acc):
    pairs = dot(split_x[...], w_ref[...])
    half = pairs.shape[1] // 2
    along_x = (pairs[:, :half] + pairs[:, half:]).T
    total = dot(jnp.concatenate(split(along_x), 0), t_ref[...])
    rows, lanes = total.shape[0] // 2, total.shape[1] // 2
    total = total[:rows] + total[rows:]
    part = total[:, :lanes] + total[:, lanes:]
    first = pl.program_id(0) == 0

    @pl.when(first)
    def _():
        acc[...] = part

    @pl.when(jnp.logical_not(first))
    def _():
        acc[...] = acc[...] + part


def modes_out(acc, out_ref, chans, modes):
    rows = acc.shape[0]
    lanes = acc.shape[1] // 2
    cosine, sine = acc[:, :lanes], acc[:, lanes:]
    halves = lanes // 128
    for c in range(chans):
        a, b, d = 2 * c * modes, (2 * c + 1) * modes, (2 * c + 2) * modes
        real = cosine[a:b] + sine[b:d]
        imag = cosine[b:d] - sine[a:b]
        for h in range(halves):
            out_ref[h * rows + a : h * rows + b] = real[:, h * 128 : (h + 1) * 128]
            out_ref[h * rows + b : h * rows + d] = imag[:, h * 128 : (h + 1) * 128]


def read_modes(ref, c, h, modes, rows):
    at = h * rows + 2 * c * modes
    return ref[at : at + modes], ref[at + modes : at + 2 * modes]


def put_modes(r_ref, c, h, modes, rows, lanes, real, imag):
    for at, value in ((0, real), (lanes, -imag)):
        for r, part in zip((0, rows), split(value)):
            r_ref[r + 2 * c * modes : r + (2 * c + 1) * modes, at + h * 128 : at + (h + 1) * 128] = part
    for at, value in ((0, imag), (lanes, real)):
        for r, part in zip((0, rows), split(value)):
            r_ref[r + (2 * c + 1) * modes : r + (2 * c + 2) * modes, at + h * 128 : at + (h + 1) * 128] = part


def synthesise(t_ref, r_ref, l_ref, spec):
    k = r_ref.shape[1]
    pairs = dot_nt(t_ref[:, :k], r_ref[...]) + dot_nt(t_ref[:, k:], r_ref[...])
    half = pairs.shape[1] // 2
    high, low = split(pairs[:, :half] + pairs[:, half:])
    spec[...] = dot(jnp.concatenate([high, low, high], 1), l_ref[...])


def kernel_a(dims, f_ref, w_ref, ty_ref, tz_ref, t_ref, u_ref, split_x, acc):
    chans, modes, ylines, zlines, ty, nx = dims
    j = pl.program_id(0)
    lanes = ty_ref.shape[1] // 2

    y0 = lax.axis_index("row") * ylines + j * ty
    z0 = pl.multiple_of(lax.axis_index("col") * zlines, zlines)

    def table(k, carry):
        ys = ty_ref[pl.ds(y0 + k, 1), :]
        zs = tz_ref[pl.ds(z0, zlines), :]
        yc, yn = ys[:, :lanes], ys[:, lanes:]
        zc, zn = zs[:, :lanes], zs[:, lanes:]
        rows = pl.ds(pl.multiple_of(k * zlines, zlines), zlines)
        for at, value in ((0, yc * zc - yn * zn), (lanes, yn * zc + yc * zn)):
            high, low = split(value)
            t_ref[rows, at : at + lanes] = high
            t_ref[rows, 2 * lanes + at : 2 * lanes + at + lanes] = low
        return carry

    lax.fori_loop(0, ty, table, 0)

    def cut(k, carry):
        rows = pl.ds(pl.multiple_of(k * zlines, zlines), zlines)
        for c in range(chans):
            high, low = split(f_ref[0, c, k])
            split_x[rows, c * nx : (c + 1) * nx] = high
            split_x[rows, (chans + c) * nx : (chans + c + 1) * nx] = low
        return carry

    lax.fori_loop(0, ty, cut, 0)
    analyse(split_x, w_ref, t_ref, acc)

    @pl.when(j == pl.num_programs(0) - 1)
    def _():
        modes_out(acc, u_ref, chans, modes)


ERFC = (0.254829592, -0.284496736, 1.421413741, -1.453152027, 1.061405429)


def gelu_slope(v):
    a = jnp.abs(v)
    t = pl.reciprocal(1.0 + (0.3275911 / math.sqrt(2.0)) * a, approx=False)
    poly = 0.5 * ERFC[4]
    for coef in ERFC[3::-1]:
        poly = poly * t + 0.5 * coef
    gauss = jnp.exp2(v * v * (-0.5 / math.log(2.0)))
    tail = gauss * (poly * t - a * (1.0 / math.sqrt(2.0 * math.pi)))
    return jnp.where(v < 0.0, tail, 1.0 - tail)


def kernel_b(dims, u_ref, sw_ref, pw_ref, b_ref, f_ref, g_ref, w_ref, l_ref, t_ref,
             h_ref, s_ref, r_ref, spec, split_x, acc):
    chans, modes, ylines, zlines, ty, nx = dims
    j = pl.program_id(0)
    lanes = t_ref.shape[1] // 4
    rows_m = acc.shape[0]

    @pl.when(j == 0)
    def _():
        for h in range(lanes // 128):
            at = slice(h * 128, (h + 1) * 128)
            for o in range(chans):
                real = imag = 0.0
                for i in range(chans):
                    ur, ui = read_modes(u_ref, i, h, modes, rows_m)
                    wr, wi = sw_ref[0, i, o, :, at], sw_ref[1, i, o, :, at]
                    real += ur * wr - ui * wi
                    imag += ur * wi + ui * wr
                put_modes(r_ref, o, h, modes, rows_m, lanes, real, imag)

    synthesise(t_ref, r_ref, l_ref, spec)
    step = 16
    per = zlines // step

    def cells(k, carry):
        y, z = k // per, k % per
        zs = pl.ds(pl.multiple_of(z * step, step), step)
        rows = pl.ds(pl.multiple_of(k * step, step), step)
        fields = [f_ref[0, i, y, zs, :] for i in range(chans)]
        for o in range(chans):
            pre = spec[rows, o * nx : (o + 1) * nx] + b_ref[o]
            for i in range(chans):
                pre += fields[i] * pw_ref[i, o]
            up = g_ref[0, o, y, zs, :] * gelu_slope(pre)
            h_ref[0, o, y, zs, :] = up
            high, low = split(up)
            split_x[rows, o * nx : (o + 1) * nx] = high
            split_x[rows, (chans + o) * nx : (chans + o + 1) * nx] = low
        return carry

    lax.fori_loop(0, ty * per, cells, 0)
    analyse(split_x, w_ref, t_ref, acc)

    @pl.when(j == pl.num_programs(0) - 1)
    def _():
        modes_out(acc, s_ref, chans, modes)


def kernel_c(dims, cells_all, u_ref, s_ref, sw_ref, pw_ref, h_ref, l_ref, t_ref,
             o_ref, gs_ref, r_ref, spec):
    chans, modes, ylines, zlines, ty, nx = dims
    j = pl.program_id(0)
    lanes = t_ref.shape[1] // 4
    rows_m = r_ref.shape[0] // 2

    @pl.when(j == 0)
    def _():
        wave = lax.broadcasted_iota(jnp.int32, (modes, 128), 0)
        factor = jnp.where(wave == 0, 1.0 / cells_all, 2.0 / cells_all).astype(f32)
        for h in range(lanes // 128):
            at = slice(h * 128, (h + 1) * 128)
            for i in range(chans):
                ur, ui = read_modes(u_ref, i, h, modes, rows_m)
                ur, ui = ur * factor, ui * factor
                real = imag = 0.0
                for o in range(chans):
                    hr, hi = read_modes(s_ref, o, h, modes, rows_m)
                    wr, wi = sw_ref[0, i, o, :, at], sw_ref[1, i, o, :, at]
                    gs_ref[0, i, o, :, at] = ur * hr + ui * hi
                    gs_ref[1, i, o, :, at] = ur * hi - ui * hr
                    real += wr * hr + wi * hi
                    imag += wr * hi - wi * hr
                put_modes(r_ref, i, h, modes, rows_m, lanes, real, imag)

    synthesise(t_ref, r_ref, l_ref, spec)
    step = 16
    per = zlines // step

    def cells(k, carry):
        y, z = k // per, k % per
        zs = pl.ds(pl.multiple_of(z * step, step), step)
        rows = pl.ds(pl.multiple_of(k * step, step), step)
        ups = [h_ref[0, o, y, zs, :] for o in range(chans)]
        for i in range(chans):
            out = spec[rows, i * nx : (i + 1) * nx]
            for o in range(chans):
                out += ups[o] * pw_ref[i, o]
            o_ref[0, i, y, zs, :] = out
        return carry

    lax.fori_loop(0, ty * per, cells, 0)


def sum_kernel(count, cols, x_ref, o_ref, got, gathered, send_a, recv_a, send_b, recv_b):
    me = lax.axis_index("row") * cols + lax.axis_index("col")

    def other(k):
        t = lax.rem(me + k, count)
        return t, {"row": t // cols, "col": lax.rem(t, cols)}

    barrier = pltpu.get_barrier_semaphore()

    def greet(k, carry):
        pl.semaphore_signal(barrier, inc=1, device_id=other(k)[1], device_id_type=MESH)
        return carry

    lax.fori_loop(1, count, greet, 0)
    pl.semaphore_wait(barrier, count - 1)

    def part(k, arriving):
        t, dev = other(k)
        slot = t if arriving else me
        return pltpu.make_async_remote_copy(
            src_ref=x_ref.at[t], dst_ref=got.at[slot], send_sem=send_a.at[t],
            recv_sem=recv_a.at[slot], device_id=dev, device_id_type=MESH)

    def whole(k, arriving):
        t, dev = other(k)
        slot = t if arriving else me
        return pltpu.make_async_remote_copy(
            src_ref=gathered.at[me], dst_ref=gathered.at[slot], send_sem=send_b.at[t],
            recv_sem=recv_b.at[slot], device_id=dev, device_id_type=MESH)

    def each(action):
        def body(k, carry):
            action(k)
            return carry
        lax.fori_loop(1, count, body, 0)

    each(lambda k: part(k, False).start())
    got[pl.ds(me, 1)] = x_ref[pl.ds(me, 1)]
    each(lambda k: part(k, True).wait_recv())
    gathered[pl.ds(me, 1)] = jnp.sum(got[...], axis=0, keepdims=True)
    each(lambda k: whole(k, False).start())
    each(lambda k: whole(k, True).wait_recv())
    o_ref[...] = gathered[...]
    each(lambda k: part(k, False).wait_send())
    each(lambda k: whole(k, False).wait_send())


def sum_modes(part, count, cols, ident):
    rows, lanes = part.shape
    shape = (count, rows // count, lanes)
    vmem = pl.BlockSpec(memory_space=pltpu.VMEM)
    out = pl.pallas_call(
        functools.partial(sum_kernel, count, cols),
        out_shape=jax.ShapeDtypeStruct(shape, f32),
        in_specs=[vmem],
        out_specs=vmem,
        scratch_shapes=[pltpu.VMEM(shape, f32), pltpu.VMEM(shape, f32)]
        + [pltpu.SemaphoreType.DMA((count,))] * 4,
        compiler_params=pltpu.CompilerParams(collective_id=ident, has_side_effects=True),
        name="sum_modes",
    )(part.reshape(shape))
    return out.reshape(rows, lanes)


def solution(mesh):
    nrow, ncol = mesh.shape["row"], mesh.shape["col"]
    count = nrow * ncol

    def per_device(fields, cotangent, spec_weights, point_weights, bias):
        _, chans, ylines, zlines, nx = fields.shape
        _, _, _, mx, my, mz = spec_weights.shape
        ny, nz = ylines * nrow, zlines * ncol
        cells_all = float(nx * ny * nz)
        lanes = my * mz
        rows_m = 2 * chans * mx
        ty = max(1, min(ylines, TILE // zlines))
        steps = ylines // ty
        tile = ty * zlines
        dims = (chans, mx, ylines, zlines, ty, nx)
        w_tab, l_tab = x_tables(chans, nx, mx, cells_all)
        y_tab, z_tab = yz_tables(ny, nz, my, mz)
        weights = spec_weights.reshape(2, chans, chans, mx, lanes)

        def keep(shape):
            return pl.BlockSpec(shape, lambda j: (0,) * len(shape))

        cells = pl.BlockSpec((1, chans, ty, zlines, nx), lambda j: (0, 0, j, 0, 0))
        table = pl.BlockSpec((tile, 4 * lanes), lambda j: (j, 0))
        smem = pl.BlockSpec(memory_space=pltpu.SMEM)
        field_shape = jax.ShapeDtypeStruct(fields.shape, f32)
        mode_shape = (rows_m * lanes // 128, 128)
        mode_out = jax.ShapeDtypeStruct(mode_shape, f32)
        x_scratch = pltpu.VMEM((tile, 2 * chans * nx), bf16)
        spec_scratch = pltpu.VMEM((tile, chans * nx), f32)
        acc_scratch = pltpu.VMEM((rows_m, 2 * lanes), f32)
        r_scratch = pltpu.VMEM((2 * rows_m, 2 * lanes), bf16)
        params = pltpu.CompilerParams(
            dimension_semantics=("arbitrary",), vmem_limit_bytes=56 * 1024 * 1024)

        t_tab, u_part = pl.pallas_call(
            functools.partial(kernel_a, dims),
            grid=(steps,),
            out_shape=(jax.ShapeDtypeStruct((ylines * zlines, 4 * lanes), bf16), mode_out),
            in_specs=[cells, keep(w_tab.shape), keep(y_tab.shape), keep(z_tab.shape)],
            out_specs=(table, keep(mode_shape)),
            scratch_shapes=[x_scratch, acc_scratch],
            compiler_params=params,
            name="analyse_fields",
        )(fields, w_tab, y_tab, z_tab)
        spectrum_u = sum_modes(u_part, count, ncol, 0)

        upstream, h_part = pl.pallas_call(
            functools.partial(kernel_b, dims),
            grid=(steps,),
            out_shape=(field_shape, mode_out),
            in_specs=[keep(mode_shape), keep(weights.shape), smem, smem, cells, cells,
                      keep(w_tab.shape), keep(l_tab.shape), table],
            out_specs=(cells, keep(mode_shape)),
            scratch_shapes=[r_scratch, spec_scratch, x_scratch, acc_scratch],
            compiler_params=params,
            name="layer_and_slope",
        )(spectrum_u, weights, point_weights, bias, fields, cotangent, w_tab, l_tab, t_tab)
        spectrum_h = sum_modes(h_part, count, ncol, 1)

        grad_fields, grad_spectral = pl.pallas_call(
            functools.partial(kernel_c, dims, cells_all),
            grid=(steps,),
            out_shape=(field_shape, jax.ShapeDtypeStruct(weights.shape, f32)),
            in_specs=[keep(mode_shape), keep(mode_shape), keep(weights.shape), smem, cells,
                      keep(l_tab.shape), table],
            out_specs=(cells, keep(weights.shape)),
            scratch_shapes=[r_scratch, spec_scratch],
            compiler_params=params,
            name="gradients",
        )(spectrum_u, spectrum_h, weights, point_weights, upstream, l_tab, t_tab)
        return grad_fields, grad_spectral.reshape(spec_weights.shape)

    placed = (P(None, None, "row", "col", None), P(None, None, "row", "col", None), P(), P(), P())
    return jax.shard_map(
        per_device,
        mesh=mesh,
        in_specs=placed,
        out_specs=(P(None, None, "row", "col", None), P()),
        check_vma=False,
    )
```
